32 devices in a mesh: row: 8 (over z, core), col: 4 (over y, x).
Axes of the slice: x: 2, y: 2, z: 4, core: 2. Of those that a mesh axis runs over, the one named last changes fastest.
Arguments:
- psi: bfloat16 [1024, 4096], P(('row', 'col')), may hold values from -6 to 6
- hpsi: bfloat16 [1024, 4096], P(('row', 'col')), may hold values from -0.1875 to 0.1875
- eigvec: bfloat16 [4, 8, 128, 8, 4, 128], P(None, 'row', None, None, 'col'), may hold values from -0.09375 to 0.09375
Outputs:
- correlation_tiles: float32 [4, 8, 128, 8, 4, 128], P(None, 'row', None, None, 'col')
- updated_tiles: float32 [4, 8, 128, 8, 4, 128], P(None, 'row', None, None, 'col')
- diag_part: float32 [16], replicated
- offdiag_part: float32 [16], replicated
- rotated: bfloat16 [1024, 8, 4, 128], P('row', None, 'col')
The draws below stay inside these ranges and needn't reach their ends.
All inputs are finite; a program needn't handle non-finite values.
Results may differ from the reference program's by a relative error of at most 0.001.
Values may be sent and summed in bfloat16 or wider, within the bound.
A program may use at most 128 MiB of HBM per device.

```python
import jax
import jax.numpy as jnp
from jax import lax

NB = 4096
TB = 128
PB = 16
NG = 1024
KR = 4
KC = 8
N_ROW = 8
N_COL = 4


def block_levels(key, shape, pieces, least, largest):
    def one(position, shards_of):
        heights = jax.random.uniform(jax.random.fold_in(jax.random.fold_in(key, 6), position), (shards_of,), jnp.float32, least / len(pieces), largest / len(pieces))
        return jnp.repeat(jnp.exp(heights), shape[position] // shards_of).reshape((-1,) + (1,) * (len(shape) - position - 1))

    loudness = one(*pieces[0])
    for cut in pieces[1:]:
        loudness = loudness * one(*cut)
    return loudness


def centred(rng, dims, spread, most, pieces=(), held_as=jnp.bfloat16):
    array = jax.random.normal(rng, dims, jnp.float32) * spread
    if len(pieces) > 0:
        array = block_levels(rng, dims, pieces, -0.22, 0.18) * array
    return jnp.clip(array, min=-most, max=most).astype(held_as)


def setup_inputs(seed: int = 0) -> dict:
    splits = jax.random.split(jax.random.key(seed), 4)
    psi = centred(splits[0], (NG, NB), 1.0, 6.0, ((0, 32),))
    hpsi = centred(splits[1], (NG, NB), NG ** -0.5, 0.1875, ((0, 32),))
    eigvec = centred(splits[2], (KR, N_ROW, TB, KC, N_COL, TB), NB ** -0.5, 0.09375, ((1, 8), (4, 4)))
    return dict(psi=psi, hpsi=hpsi, eigvec=eigvec)


def reference(psi, hpsi, eigvec):
    highest = lax.Precision.HIGHEST
    mixed = jnp.dot(psi.T, hpsi, preferred_element_type=jnp.float32)
    reduced = 0.5 * (mixed + mixed.T)
    correlation = jnp.dot(psi.T, psi, preferred_element_type=jnp.float32) / float(NG)
    panel = reduced[:, :PB]
    positions = jnp.arange(NB)
    vecs = jnp.zeros((NB, PB), jnp.float32)
    images = jnp.zeros((NB, PB), jnp.float32)
    diag_list = []
    off_list = []
    for step in range(PB):
        column = panel[:, step] - jnp.dot(vecs, images[step], precision=highest) - jnp.dot(images, vecs[step], precision=highest)
        pivot = column[step + 1]
        below = positions > step + 1
        tail = jnp.sum(jnp.where(below, column * column, 0.0))
        length = jnp.sqrt(pivot * pivot + tail)
        beta = jnp.where(pivot >= 0.0, -length, length)
        tau = (beta - pivot) / beta
        vector = jnp.where(positions == step + 1, 1.0, jnp.where(below, column / (pivot - beta), 0.0))
        image = jnp.dot(reduced, vector, precision=highest)
        image = image - jnp.dot(vecs, jnp.dot(vector, images, precision=highest), precision=highest)
        image = image - jnp.dot(images, jnp.dot(vector, vecs, precision=highest), precision=highest)
        image = tau * image
        image = image - 0.5 * tau * jnp.dot(image, vector, precision=highest) * vector
        vecs = vecs.at[:, step].set(vector)
        images = images.at[:, step].set(image)
        diag_list.append(column[step])
        off_list.append(beta)
    updated = reduced - jnp.dot(vecs, images.T, precision=highest) - jnp.dot(images, vecs.T, precision=highest)
    rotation = eigvec.reshape(NB, NB)
    rotated = jnp.dot(psi, rotation, preferred_element_type=jnp.float32).astype(jnp.bfloat16)
    tile_shape = (KR, N_ROW, TB, KC, N_COL, TB)
    return (correlation.reshape(tile_shape), updated.reshape(tile_shape), jnp.stack(diag_list).astype(jnp.float32), jnp.stack(off_list).astype(jnp.float32), rotated.reshape(NG, KC, N_COL, TB))
```

```python
import functools

import jax
import jax.numpy as jnp
from jax import lax
from jax.experimental import pallas as pl
from jax.experimental.pallas import tpu as pltpu
from jax.sharding import PartitionSpec as P

PB = 16


def inner(left, right):
    return lax.dot_general(
        left, right, (((0,), (0,)), ((), ())), preferred_element_type=jnp.float32
    )


def total(array):
    return jnp.sum(array, axis=(0, 1), keepdims=True)


def panel_kernel(
    sizes, block, lead, vecs, images, diagonal, offdiag,
    panel, places, vector_now, folded, part, piece, gathered, full,
    lead_part, lead_piece, lead_all, col_send, col_recv, row_send, row_recv,
):
    row_count, col_count, row_tiles, col_tiles, tile = sizes
    row_id = lax.axis_index("row")
    col_id = lax.axis_index("col")

    def col_peer(distance):
        return (row_id, lax.rem(col_id + distance, col_count))

    def row_peer(distance):
        return (lax.rem(row_id + distance, row_count), col_id)

    barrier = pltpu.get_barrier_semaphore()
    for distance in range(1, col_count):
        pl.semaphore_signal(
            barrier, inc=1, device_id=col_peer(distance), device_id_type=pl.DeviceIdType.MESH
        )
    for distance in range(1, row_count):
        pl.semaphore_signal(
            barrier, inc=1, device_id=row_peer(distance), device_id_type=pl.DeviceIdType.MESH
        )
    pl.semaphore_wait(barrier, row_count + col_count - 2)

    def col_copies(source, target, slot):
        return [
            pltpu.make_async_remote_copy(
                src_ref=source,
                dst_ref=target,
                send_sem=col_send.at[slot, distance],
                recv_sem=col_recv.at[slot, distance],
                device_id=col_peer(distance),
                device_id_type=pl.DeviceIdType.MESH,
            )
            for distance in range(1, col_count)
        ]

    def row_copies(source, target, slot):
        return [
            pltpu.make_async_remote_copy(
                src_ref=source,
                dst_ref=target,
                send_sem=row_send.at[slot, distance],
                recv_sem=row_recv.at[slot, distance],
                device_id=row_peer(distance),
                device_id_type=pl.DeviceIdType.MESH,
            )
            for distance in range(1, row_count)
        ]

    copies = col_copies(lead, lead_part.at[col_id], 2)
    for copy in copies:
        copy.start()
    lead_part[pl.ds(col_id, 1)] = lead[...][None]
    vecs[...] = jnp.zeros_like(vecs)
    images[...] = jnp.zeros_like(images)
    diagonal[...] = jnp.zeros_like(diagonal)
    offdiag[...] = jnp.zeros_like(offdiag)
    lanes = lax.broadcasted_iota(jnp.int32, (row_tiles, tile), 1)
    tiles = lax.broadcasted_iota(jnp.int32, (row_tiles, tile), 0)
    for owner in range(row_count):
        places[owner * row_tiles : (owner + 1) * row_tiles, :] = (
            tiles * row_count + owner
        ) * tile + lanes
    for copy in copies:
        copy.wait()
    summed = lead_part[0]
    for source in range(1, col_count):
        summed = summed + lead_part[source]
    lead_piece[...] = summed
    copies = row_copies(lead_piece, lead_all.at[row_id], 2)
    for copy in copies:
        copy.start()
    lead_all[pl.ds(row_id, 1)] = summed[None]
    for copy in copies:
        copy.wait()
    for owner in range(row_count):
        panel[:, owner * row_tiles : (owner + 1) * row_tiles, :] = lead_all[owner]

    pos = places[...]
    lane = lax.broadcasted_iota(jnp.int32, (1, tile), 1)
    lane3 = lax.broadcasted_iota(jnp.int32, (PB, 1, tile), 2)
    chunk = 64
    rows = row_tiles * tile

    @pl.loop(0, PB)
    def _(step):
        slot = lax.rem(step, 2)
        head_v = jnp.sum(jnp.where(lane3 == step, vecs[:, 0:1, :], 0.0), axis=2, keepdims=True)
        head_w = jnp.sum(jnp.where(lane3 == step, images[:, 0:1, :], 0.0), axis=2, keepdims=True)
        column = panel[step]
        for k in range(PB - 1):
            column = column - vecs[k] * head_w[k] - images[k] * head_v[k]
        below = pos > step + 1
        pivot = total(jnp.where(pos == step + 1, column, 0.0))
        here = total(jnp.where(pos == step, column, 0.0))
        tail = total(jnp.where(below, column * column, 0.0))
        length = jnp.sqrt(pivot * pivot + tail)
        beta = jnp.where(pivot >= 0.0, -length, length)
        tau = (beta - pivot) / beta
        vector = jnp.where(
            pos == step + 1, 1.0, jnp.where(below, column / (pivot - beta), 0.0)
        )
        vector_now[...] = vector
        local = []
        for g in range(col_tiles):
            b = col_id + col_count * g
            local.append(
                vector_now[pl.ds(lax.rem(b, row_count) * row_tiles + lax.div(b, row_count), 1), :]
            )
        for start in range(0, rows, chunk):
            acc = block[start : start + chunk, 0:tile] * local[0]
            for g in range(1, col_tiles):
                acc = acc + block[start : start + chunk, g * tile : (g + 1) * tile] * local[g]
            folded[start : start + chunk, :] = acc
        sums = lax.dot_general(
            jnp.ones((8, tile), jnp.float32),
            folded[...],
            (((1,), (1,)), ((), ())),
            precision=lax.Precision.HIGHEST,
            preferred_element_type=jnp.float32,
        )
        for t in range(row_tiles):
            part[step, col_id, t : t + 1, :] = sums[0:1, t * tile : (t + 1) * tile]
        sent = col_copies(part.at[step, col_id], part.at[step, col_id], slot)
        for copy in sent:
            copy.start()
        onto_w = [total(images[k] * vector) for k in range(PB - 1)]
        onto_v = [total(vecs[k] * vector) for k in range(PB - 1)]
        fix = vecs[0] * onto_w[0] + images[0] * onto_v[0]
        for k in range(1, PB - 1):
            fix = fix + vecs[k] * onto_w[k] + images[k] * onto_v[k]
        vecs[pl.ds(step, 1)] = vector[None]
        diagonal[...] = jnp.where(lane == step, here, diagonal[...])
        offdiag[...] = jnp.where(lane == step, beta, offdiag[...])
        for copy in sent:
            copy.wait()
        image = part[step, 0]
        for source in range(1, col_count):
            image = image + part[step, source]
        gathered[step, row_id] = image
        sent = row_copies(gathered.at[step, row_id], gathered.at[step, row_id], slot)
        for copy in sent:
            copy.start()
        for copy in sent:
            copy.wait()
        for owner in range(row_count):
            full[owner * row_tiles : (owner + 1) * row_tiles, :] = gathered[step, owner]
        image = tau * (full[...] - fix)
        image = image - 0.5 * tau * total(image * vector) * vector
        images[pl.ds(step, 1)] = image[None]


def reduce_panel(block, lead, sizes):
    row_count, col_count, row_tiles, col_tiles, tile = sizes
    all_tiles = row_count * row_tiles
    f32 = jnp.float32
    whole = pl.BlockSpec(memory_space=pltpu.VMEM)
    return pl.pallas_call(
        functools.partial(panel_kernel, sizes),
        out_shape=(
            jax.ShapeDtypeStruct((PB, all_tiles, tile), f32),
            jax.ShapeDtypeStruct((PB, all_tiles, tile), f32),
            jax.ShapeDtypeStruct((1, tile), f32),
            jax.ShapeDtypeStruct((1, tile), f32),
        ),
        in_specs=[whole, whole],
        out_specs=(whole, whole, whole, whole),
        scratch_shapes=[
            pltpu.VMEM((PB, all_tiles, tile), f32),
            pltpu.VMEM((all_tiles, tile), jnp.int32),
            pltpu.VMEM((all_tiles, tile), f32),
            pltpu.VMEM((row_tiles * tile, tile), f32),
            pltpu.VMEM((PB, col_count, row_tiles, tile), f32),
            pltpu.VMEM((row_tiles, tile), f32),
            pltpu.VMEM((PB, row_count, row_tiles, tile), f32),
            pltpu.VMEM((all_tiles, tile), f32),
            pltpu.VMEM((col_count, PB, row_tiles, tile), f32),
            pltpu.VMEM((PB, row_tiles, tile), f32),
            pltpu.VMEM((row_count, PB, row_tiles, tile), f32),
            pltpu.SemaphoreType.DMA((3, col_count)),
            pltpu.SemaphoreType.DMA((3, col_count)),
            pltpu.SemaphoreType.DMA((3, row_count)),
            pltpu.SemaphoreType.DMA((3, row_count)),
        ],
        compiler_params=pltpu.CompilerParams(
            collective_id=0, has_side_effects=True, vmem_limit_bytes=24 * 1024 * 1024
        ),
        cost_estimate=pl.CostEstimate(
            flops=400_000_000, bytes_accessed=4_000_000, transcendentals=0
        ),
        name="panel",
    )(block, lead)


def on_device(psi, hpsi, eigvec):
    highest = lax.Precision.HIGHEST
    g_rows = psi.shape[0]
    bands = psi.shape[1]
    row_tiles = eigvec.shape[0]
    tile_size = eigvec.shape[2]
    col_tiles = eigvec.shape[3]
    row_count = lax.axis_size("row")
    col_count = lax.axis_size("col")
    row_id = lax.axis_index("row")
    col_id = lax.axis_index("col")
    gvecs = g_rows * row_count * col_count
    row_width = row_tiles * tile_size
    col_width = col_tiles * tile_size
    lifted = (
        psi.reshape(1, g_rows, row_tiles, row_count, tile_size),
        hpsi.reshape(1, g_rows, row_tiles, row_count, tile_size),
    )
    swapped = (
        lax.all_to_all(lifted[0], "row", split_axis=3, concat_axis=0, tiled=True),
        lax.all_to_all(lifted[1], "row", split_axis=3, concat_axis=0, tiled=True),
    )
    joined = (
        lax.all_gather(swapped[0], "col", axis=1, tiled=True),
        lax.all_gather(swapped[1], "col", axis=1, tiled=True),
    )
    psi_rows = joined[0].reshape(gvecs, row_width)
    hpsi_rows = joined[1].reshape(gvecs, row_width)
    lowered = (
        psi.reshape(g_rows, col_tiles, col_count, tile_size),
        hpsi.reshape(g_rows, col_tiles, col_count, tile_size),
    )
    moved = (
        lax.all_to_all(lowered[0], "col", split_axis=2, concat_axis=0, tiled=True),
        lax.all_to_all(lowered[1], "col", split_axis=2, concat_axis=0, tiled=True),
    )
    stacked = (
        lax.all_gather(moved[0], "row", axis=0, tiled=True),
        lax.all_gather(moved[1], "row", axis=0, tiled=True),
    )
    psi_cols = stacked[0].reshape(gvecs, col_width)
    hpsi_cols = stacked[1].reshape(gvecs, col_width)
    reduced = 0.5 * (inner(psi_rows, hpsi_cols) + inner(hpsi_rows, psi_cols))
    correlation = inner(psi_rows, psi_cols) / float(gvecs)
    blocks = reduced.reshape(row_tiles, tile_size, col_tiles, tile_size)
    leading = blocks[:, :, 0, :PB]
    lead = jnp.where(col_id == 0, jnp.transpose(leading, (2, 0, 1)), 0.0)
    sizes = (row_count, col_count, row_tiles, col_tiles, tile_size)
    vecs, images, diagonal, offdiag = reduce_panel(reduced, lead, sizes)
    diagonal = diagonal[0, :PB]
    offdiag = offdiag[0, :PB]

    def rows_of(matrix):
        return lax.dynamic_index_in_dim(
            matrix.reshape(PB, row_count, row_tiles, tile_size), row_id, 1, keepdims=False
        ).reshape(PB, row_width)

    def cols_of(matrix):
        ordered = jnp.transpose(
            matrix.reshape(PB, row_count, row_tiles, tile_size), (0, 2, 1, 3)
        )
        return lax.dynamic_index_in_dim(
            ordered.reshape(PB, col_tiles, col_count, tile_size), col_id, 2, keepdims=False
        ).reshape(PB, col_width)

    left = jnp.concatenate([rows_of(vecs), rows_of(images)], axis=0)
    right = jnp.concatenate([cols_of(images), cols_of(vecs)], axis=0)
    updated = reduced - lax.dot_general(
        left, right, (((0,), (0,)), ((), ())), precision=highest,
        preferred_element_type=jnp.float32,
    )
    flat = eigvec.reshape(row_width, col_width)
    rotated = lax.psum_scatter(
        jnp.dot(psi_rows, flat, preferred_element_type=jnp.float32),
        "row",
        scatter_dimension=0,
        tiled=True,
    )
    tile_shape = (row_tiles, 1, tile_size, col_tiles, 1, tile_size)
    return (
        correlation.reshape(tile_shape),
        updated.reshape(tile_shape),
        diagonal,
        offdiag,
        rotated.astype(jnp.bfloat16).reshape(rotated.shape[0], col_tiles, 1, tile_size),
    )


def solution(mesh):
    return jax.shard_map(
        on_device,
        mesh=mesh,
        in_specs=(
            P(("row", "col"), None),
            P(("row", "col"), None),
            P(None, "row", None, None, "col", None),
        ),
        out_specs=(
            P(None, "row", None, None, "col", None),
            P(None, "row", None, None, "col", None),
            P(),
            P(),
            P("row", None, "col", None),
        ),
        check_vma=False,
    )
```

```python
import functools

import jax
import jax.numpy as jnp
from jax import lax
from jax.experimental import pallas as pl
from jax.experimental.pallas import tpu as pltpu
from jax.sharding import PartitionSpec as P

PB = 16


def inner(left, right):
    return lax.dot_general(
        left, right, (((0,), (0,)), ((), ())), preferred_element_type=jnp.float32
    )


def total(array):
    return jnp.sum(array, axis=(0, 1), keepdims=True)


def panel_kernel(
    sizes, block, lead, vecs, images, diagonal, offdiag,
    panel, places, vector_now, folded, part, piece, gathered, full,
    lead_part, lead_piece, lead_all, col_send, col_recv, row_send, row_recv,
):
    row_count, col_count, row_tiles, col_tiles, tile = sizes
    row_id = lax.axis_index("row")
    col_id = lax.axis_index("col")

    def col_peer(distance):
        return (row_id, lax.rem(col_id + distance, col_count))

    def row_peer(distance):
        return (lax.rem(row_id + distance, row_count), col_id)

    barrier = pltpu.get_barrier_semaphore()
    for distance in range(1, col_count):
        pl.semaphore_signal(
            barrier, inc=1, device_id=col_peer(distance), device_id_type=pl.DeviceIdType.MESH
        )
    for distance in range(1, row_count):
        pl.semaphore_signal(
            barrier, inc=1, device_id=row_peer(distance), device_id_type=pl.DeviceIdType.MESH
        )
    pl.semaphore_wait(barrier, row_count + col_count - 2)

    def col_copies(source, target, slot):
        return [
            pltpu.make_async_remote_copy(
                src_ref=source,
                dst_ref=target,
                send_sem=col_send.at[slot, distance],
                recv_sem=col_recv.at[slot, distance],
                device_id=col_peer(distance),
                device_id_type=pl.DeviceIdType.MESH,
            )
            for distance in range(1, col_count)
        ]

    def row_copies(source, target, slot):
        return [
            pltpu.make_async_remote_copy(
                src_ref=source,
                dst_ref=target,
                send_sem=row_send.at[slot, distance],
                recv_sem=row_recv.at[slot, distance],
                device_id=row_peer(distance),
                device_id_type=pl.DeviceIdType.MESH,
            )
            for distance in range(1, row_count)
        ]

    copies = col_copies(lead, lead_part.at[col_id], 2)
    for copy in copies:
        copy.start()
    lead_part[pl.ds(col_id, 1)] = lead[...][None]
    vecs[...] = jnp.zeros_like(vecs)
    images[...] = jnp.zeros_like(images)
    diagonal[...] = jnp.zeros_like(diagonal)
    offdiag[...] = jnp.zeros_like(offdiag)
    lanes = lax.broadcasted_iota(jnp.int32, (row_tiles, tile), 1)
    tiles = lax.broadcasted_iota(jnp.int32, (row_tiles, tile), 0)
    for owner in range(row_count):
        places[owner * row_tiles : (owner + 1) * row_tiles, :] = (
            tiles * row_count + owner
        ) * tile + lanes
    for copy in copies:
        copy.wait()
    summed = lead_part[0]
    for source in range(1, col_count):
        summed = summed + lead_part[source]
    lead_piece[...] = summed
    copies = row_copies(lead_piece, lead_all.at[row_id], 2)
    for copy in copies:
        copy.start()
    lead_all[pl.ds(row_id, 1)] = summed[None]
    for copy in copies:
        copy.wait()
    for owner in range(row_count):
        panel[:, owner * row_tiles : (owner + 1) * row_tiles, :] = lead_all[owner]

    pos = places[...]
    lane = lax.broadcasted_iota(jnp.int32, (1, tile), 1)
    lane3 = lax.broadcasted_iota(jnp.int32, (PB, 1, tile), 2)
    chunk = 64
    rows = row_tiles * tile

    @pl.loop(0, PB)
    def _(step):
        slot = lax.rem(step, 2)
        head_v = jnp.sum(jnp.where(lane3 == step, vecs[:, 0:1, :], 0.0), axis=2, keepdims=True)
        head_w = jnp.sum(jnp.where(lane3 == step, images[:, 0:1, :], 0.0), axis=2, keepdims=True)
        column = panel[step]
        for k in range(PB - 1):
            column = column - vecs[k] * head_w[k] - images[k] * head_v[k]
        below = pos > step + 1
        pivot = total(jnp.where(pos == step + 1, column, 0.0))
        here = total(jnp.where(pos == step, column, 0.0))
        tail = total(jnp.where(below, column * column, 0.0))
        length = jnp.sqrt(pivot * pivot + tail)
        beta = jnp.where(pivot >= 0.0, -length, length)
        tau = (beta - pivot) / beta
        vector = jnp.where(
            pos == step + 1, 1.0, jnp.where(below, column / (pivot - beta), 0.0)
        )
        vector_now[...] = vector
        local = []
        for g in range(col_tiles):
            b = col_id + col_count * g
            local.append(
                vector_now[pl.ds(lax.rem(b, row_count) * row_tiles + lax.div(b, row_count), 1), :]
            )
        for start in range(0, rows, chunk):
            acc = block[start : start + chunk, 0:tile] * local[0]
            for g in range(1, col_tiles):
                acc = acc + block[start : start + chunk, g * tile : (g + 1) * tile] * local[g]
            folded[start : start + chunk, :] = acc
        sums = lax.dot_general(
            jnp.ones((8, tile), jnp.float32),
            folded[...],
            (((1,), (1,)), ((), ())),
            precision=lax.Precision.HIGHEST,
            preferred_element_type=jnp.float32,
        )
        for t in range(row_tiles):
            part[step, col_id, t : t + 1, :] = sums[0:1, t * tile : (t + 1) * tile]
        sent = col_copies(part.at[step, col_id], part.at[step, col_id], slot)
        for copy in sent:
            copy.start()
        onto_w = [total(images[k] * vector) for k in range(PB - 1)]
        onto_v = [total(vecs[k] * vector) for k in range(PB - 1)]
        fix = vecs[0] * onto_w[0] + images[0] * onto_v[0]
        for k in range(1, PB - 1):
            fix = fix + vecs[k] * onto_w[k] + images[k] * onto_v[k]
        vecs[pl.ds(step, 1)] = vector[None]
        diagonal[...] = jnp.where(lane == step, here, diagonal[...])
        offdiag[...] = jnp.where(lane == step, beta, offdiag[...])
        for copy in sent:
            copy.wait()
        image = part[step, 0]
        for source in range(1, col_count):
            image = image + part[step, source]
        gathered[step, row_id] = image
        sent = row_copies(gathered.at[step, row_id], gathered.at[step, row_id], slot)
        for copy in sent:
            copy.start()
        for copy in sent:
            copy.wait()
        for owner in range(row_count):
            full[owner * row_tiles : (owner + 1) * row_tiles, :] = gathered[step, owner]
        image = tau * (full[...] - fix)
        image = image - 0.5 * tau * total(image * vector) * vector
        images[pl.ds(step, 1)] = image[None]


def reduce_panel(block, lead, sizes):
    row_count, col_count, row_tiles, col_tiles, tile = sizes
    all_tiles = row_count * row_tiles
    f32 = jnp.float32
    whole = pl.BlockSpec(memory_space=pltpu.VMEM)
    return pl.pallas_call(
        functools.partial(panel_kernel, sizes),
        out_shape=(
            jax.ShapeDtypeStruct((PB, all_tiles, tile), f32),
            jax.ShapeDtypeStruct((PB, all_tiles, tile), f32),
            jax.ShapeDtypeStruct((1, tile), f32),
            jax.ShapeDtypeStruct((1, tile), f32),
        ),
        in_specs=[whole, whole],
        out_specs=(whole, whole, whole, whole),
        scratch_shapes=[
            pltpu.VMEM((PB, all_tiles, tile), f32),
            pltpu.VMEM((all_tiles, tile), jnp.int32),
            pltpu.VMEM((all_tiles, tile), f32),
            pltpu.VMEM((row_tiles * tile, tile), f32),
            pltpu.VMEM((PB, col_count, row_tiles, tile), f32),
            pltpu.VMEM((row_tiles, tile), f32),
            pltpu.VMEM((PB, row_count, row_tiles, tile), f32),
            pltpu.VMEM((all_tiles, tile), f32),
            pltpu.VMEM((col_count, PB, row_tiles, tile), f32),
            pltpu.VMEM((PB, row_tiles, tile), f32),
            pltpu.VMEM((row_count, PB, row_tiles, tile), f32),
            pltpu.SemaphoreType.DMA((3, col_count)),
            pltpu.SemaphoreType.DMA((3, col_count)),
            pltpu.SemaphoreType.DMA((3, row_count)),
            pltpu.SemaphoreType.DMA((3, row_count)),
        ],
        compiler_params=pltpu.CompilerParams(
            collective_id=0, has_side_effects=True, vmem_limit_bytes=24 * 1024 * 1024
        ),
        cost_estimate=pl.CostEstimate(
            flops=400_000_000, bytes_accessed=4_000_000, transcendentals=0
        ),
        name="panel",
    )(block, lead)


def spread_kernel(
    row_count, col_count, rows_in, cols_in, row_all, col_all,
    own_sem, a1_send, a1_recv, a2_send, a2_recv, b1_send, b1_recv,
    right_send, right_recv, left_send, left_recv, pair_send, pair_recv,
):
    row_id = lax.axis_index("row")
    col_id = lax.axis_index("col")
    ring = row_count // 2
    half = ring // 2

    def row_at(shift):
        return lax.rem(row_id + shift + row_count, row_count)

    def col_peer(distance):
        return (row_id, lax.rem(col_id + distance, col_count))

    barrier = pltpu.get_barrier_semaphore()
    for distance in range(1, col_count):
        pl.semaphore_signal(
            barrier, inc=1, device_id=col_peer(distance), device_id_type=pl.DeviceIdType.MESH
        )
    for distance in range(1, row_count):
        pl.semaphore_signal(
            barrier, inc=1, device_id=(row_at(distance), col_id),
            device_id_type=pl.DeviceIdType.MESH,
        )
    pl.semaphore_wait(barrier, row_count + col_count - 2)

    def remote(source, target, send, recv, device):
        return pltpu.make_async_remote_copy(
            src_ref=source, dst_ref=target, send_sem=send, recv_sem=recv,
            device_id=device, device_id_type=pl.DeviceIdType.MESH,
        )

    own = [
        pltpu.make_async_copy(cols_in.at[col_id], col_all.at[:, row_id, col_id], own_sem.at[0]),
        pltpu.make_async_copy(rows_in.at[row_id], row_all.at[:, row_id, col_id], own_sem.at[1]),
    ]
    b1 = []
    for d in range(1, col_count):
        peer = col_peer(d)
        b1.append(remote(
            cols_in.at[peer[1]], col_all.at[:, row_id, col_id], b1_send.at[d], b1_recv.at[d], peer
        ))
    a1 = []
    for d in range(1, row_count):
        peer = row_at(d)
        a1.append(remote(
            rows_in.at[peer], row_all.at[:, row_id, col_id], a1_send.at[d], a1_recv.at[d],
            (peer, col_id),
        ))
    for copy in b1 + own + a1:
        copy.start()
    own[0].wait()
    for copy in b1:
        copy.wait()

    def forward(step, origin, shift, final_part, send, recv):
        place = col_all.at[:, origin] if step < half else col_all.at[final_part, origin]
        return remote(place, place, send.at[step], recv.at[step], (row_at(shift), col_id))

    partner = row_id + 1 - 2 * lax.rem(row_id, 2)

    def to_partner(index, origin):
        place = col_all.at[:, origin]
        return remote(place, place, pair_send.at[index], pair_recv.at[index], (partner, col_id))

    right = [forward(1, row_id, 2, 0, right_send, right_recv)]
    left = [forward(1, row_id, -2, 1, left_send, left_recv)]
    pairs = [to_partner(0, row_id)]
    right[0].start()
    left[0].start()
    pairs[0].start()
    own[1].wait()
    for copy in a1:
        copy.wait()
    a2 = []
    for d in range(1, col_count):
        place = row_all.at[:, :, col_id]
        a2.append(remote(place, place, a2_send.at[d], a2_recv.at[d], col_peer(d)))
        a2[-1].start()
    for step in range(1, half):
        from_left = row_at(-2 * step)
        from_right = row_at(2 * step)
        right[-1].wait_recv()
        right.append(forward(step + 1, from_left, 2, 0, right_send, right_recv))
        right[-1].start()
        left[-1].wait_recv()
        left.append(forward(step + 1, from_right, -2, 1, left_send, left_recv))
        left[-1].start()
        for index, origin in ((2 * step - 1, from_left), (2 * step, from_right)):
            pairs.append(to_partner(index, origin))
            pairs[-1].start()
    right[-1].wait_recv()
    left[-1].wait_recv()
    pairs.append(to_partner(ring - 1, row_at(2 * half)))
    pairs[-1].start()
    for copy in a2:
        copy.wait()
    for copy in pairs:
        copy.wait()
    for copy in right + left:
        copy.wait_send()


def spread(psi, hpsi, row_count, col_count, row_tiles, col_tiles, tile):
    g_rows = psi.shape[0]
    both = jnp.stack([psi, hpsi])
    rows_in = jnp.transpose(
        both.reshape(2, g_rows, row_tiles, row_count, tile), (3, 0, 1, 2, 4)
    ).reshape(row_count, 2, g_rows, row_tiles * tile)
    cols_in = jnp.transpose(
        both.reshape(2, g_rows, col_tiles, col_count, tile), (3, 0, 1, 2, 4)
    ).reshape(col_count, 2, g_rows, col_tiles * tile)
    whole = pl.BlockSpec(memory_space=pltpu.VMEM)
    hbm = pl.BlockSpec(memory_space=pltpu.VMEM)
    ring = row_count // 2
    dma = pltpu.SemaphoreType.DMA
    return pl.pallas_call(
        functools.partial(spread_kernel, row_count, col_count),
        out_shape=(
            jax.ShapeDtypeStruct(
                (2, row_count, col_count, g_rows, row_tiles * tile), psi.dtype
            ),
            jax.ShapeDtypeStruct(
                (2, row_count, col_count, g_rows, col_tiles * tile), psi.dtype
            ),
        ),
        in_specs=[whole, whole],
        out_specs=(hbm, hbm),
        scratch_shapes=[
            dma((2,)),
            dma((row_count,)), dma((row_count,)),
            dma((col_count,)), dma((col_count,)),
            dma((col_count,)), dma((col_count,)),
            dma((ring,)), dma((ring,)), dma((ring,)), dma((ring,)),
            dma((ring,)), dma((ring,)),
        ],
        compiler_params=pltpu.CompilerParams(
            collective_id=1, has_side_effects=True, vmem_limit_bytes=40 * 1024 * 1024
        ),
        cost_estimate=pl.CostEstimate(
            flops=100_000_000, bytes_accessed=8_000_000, transcendentals=0
        ),
        name="spread",
    )(rows_in, cols_in)


def on_device(psi, hpsi, eigvec):
    highest = lax.Precision.HIGHEST
    g_rows = psi.shape[0]
    bands = psi.shape[1]
    row_tiles = eigvec.shape[0]
    tile_size = eigvec.shape[2]
    col_tiles = eigvec.shape[3]
    row_count = lax.axis_size("row")
    col_count = lax.axis_size("col")
    row_id = lax.axis_index("row")
    col_id = lax.axis_index("col")
    gvecs = g_rows * row_count * col_count
    row_width = row_tiles * tile_size
    col_width = col_tiles * tile_size
    row_all, col_all = spread(
        psi, hpsi, row_count, col_count, row_tiles, col_tiles, tile_size
    )
    psi_rows = row_all[0].reshape(gvecs, row_width)
    hpsi_rows = row_all[1].reshape(gvecs, row_width)
    psi_cols = col_all[0].reshape(gvecs, col_width)
    hpsi_cols = col_all[1].reshape(gvecs, col_width)
    reduced = 0.5 * (inner(psi_rows, hpsi_cols) + inner(hpsi_rows, psi_cols))
    correlation = inner(psi_rows, psi_cols) / float(gvecs)
    blocks = reduced.reshape(row_tiles, tile_size, col_tiles, tile_size)
    leading = blocks[:, :, 0, :PB]
    lead = jnp.where(col_id == 0, jnp.transpose(leading, (2, 0, 1)), 0.0)
    sizes = (row_count, col_count, row_tiles, col_tiles, tile_size)
    vecs, images, diagonal, offdiag = reduce_panel(reduced, lead, sizes)
    diagonal = diagonal[0, :PB]
    offdiag = offdiag[0, :PB]

    def rows_of(matrix):
        return lax.dynamic_index_in_dim(
            matrix.reshape(PB, row_count, row_tiles, tile_size), row_id, 1, keepdims=False
        ).reshape(PB, row_width)

    def cols_of(matrix):
        ordered = jnp.transpose(
            matrix.reshape(PB, row_count, row_tiles, tile_size), (0, 2, 1, 3)
        )
        return lax.dynamic_index_in_dim(
            ordered.reshape(PB, col_tiles, col_count, tile_size), col_id, 2, keepdims=False
        ).reshape(PB, col_width)

    left = jnp.concatenate([rows_of(vecs), rows_of(images)], axis=0)
    right = jnp.concatenate([cols_of(images), cols_of(vecs)], axis=0)
    updated = reduced - lax.dot_general(
        left, right, (((0,), (0,)), ((), ())), precision=highest,
        preferred_element_type=jnp.float32,
    )
    flat = eigvec.reshape(row_width, col_width)
    rotated = lax.psum_scatter(
        jnp.dot(psi_rows, flat, preferred_element_type=jnp.float32),
        "row",
        scatter_dimension=0,
        tiled=True,
    )
    tile_shape = (row_tiles, 1, tile_size, col_tiles, 1, tile_size)
    return (
        correlation.reshape(tile_shape),
        updated.reshape(tile_shape),
        diagonal,
        offdiag,
        rotated.astype(jnp.bfloat16).reshape(rotated.shape[0], col_tiles, 1, tile_size),
    )


def solution(mesh):
    return jax.shard_map(
        on_device,
        mesh=mesh,
        in_specs=(
            P(("row", "col"), None),
            P(("row", "col"), None),
            P(None, "row", None, None, "col", None),
        ),
        out_specs=(
            P(None, "row", None, None, "col", None),
            P(None, "row", None, None, "col", None),
            P(),
            P(),
            P("row", None, "col", None),
        ),
        check_vma=False,
    )
```

```python
import functools

import jax
import jax.numpy as jnp
from jax import lax
from jax.experimental import pallas as pl
from jax.experimental.pallas import tpu as pltpu
from jax.sharding import PartitionSpec as P

PB = 16


def inner(left, right):
    return lax.dot_general(
        left, right, (((0,), (0,)), ((), ())), preferred_element_type=jnp.float32
    )


def total(array):
    return jnp.sum(array, axis=(0, 1), keepdims=True)


def panel_kernel(
    sizes, block, lead, vecs, images, diagonal, offdiag,
    panel, places, vector_now, folded, part, full,
    lead_part, lead_piece, lead_all, col_send, col_recv, row_send, row_recv,
    all_send, all_recv,
):
    row_count, col_count, row_tiles, col_tiles, tile = sizes
    row_id = lax.axis_index("row")
    col_id = lax.axis_index("col")

    def col_peer(distance):
        return (row_id, lax.rem(col_id + distance, col_count))

    def row_peer(distance):
        return (lax.rem(row_id + distance, row_count), col_id)

    devices = row_count * col_count
    flat_id = row_id * col_count + col_id

    def any_peer(distance):
        flat = lax.rem(flat_id + distance, devices)
        return (lax.div(flat, col_count), lax.rem(flat, col_count))

    barrier = pltpu.get_barrier_semaphore()
    for distance in range(1, devices):
        pl.semaphore_signal(
            barrier, inc=1, device_id=any_peer(distance), device_id_type=pl.DeviceIdType.MESH
        )
    pl.semaphore_wait(barrier, devices - 1)

    def all_copies(place, slot):
        return [
            pltpu.make_async_remote_copy(
                src_ref=place,
                dst_ref=place,
                send_sem=all_send.at[slot, distance],
                recv_sem=all_recv.at[slot, distance],
                device_id=any_peer(distance),
                device_id_type=pl.DeviceIdType.MESH,
            )
            for distance in range(1, devices)
        ]

    def col_copies(source, target):
        return [
            pltpu.make_async_remote_copy(
                src_ref=source,
                dst_ref=target,
                send_sem=col_send.at[distance],
                recv_sem=col_recv.at[distance],
                device_id=col_peer(distance),
                device_id_type=pl.DeviceIdType.MESH,
            )
            for distance in range(1, col_count)
        ]

    def row_copies(source, target):
        return [
            pltpu.make_async_remote_copy(
                src_ref=source,
                dst_ref=target,
                send_sem=row_send.at[distance],
                recv_sem=row_recv.at[distance],
                device_id=row_peer(distance),
                device_id_type=pl.DeviceIdType.MESH,
            )
            for distance in range(1, row_count)
        ]

    copies = col_copies(lead, lead_part.at[col_id])
    for copy in copies:
        copy.start()
    lead_part[pl.ds(col_id, 1)] = lead[...][None]
    vecs[...] = jnp.zeros_like(vecs)
    images[...] = jnp.zeros_like(images)
    diagonal[...] = jnp.zeros_like(diagonal)
    offdiag[...] = jnp.zeros_like(offdiag)
    lanes = lax.broadcasted_iota(jnp.int32, (row_tiles, tile), 1)
    tiles = lax.broadcasted_iota(jnp.int32, (row_tiles, tile), 0)
    for owner in range(row_count):
        places[owner * row_tiles : (owner + 1) * row_tiles, :] = (
            tiles * row_count + owner
        ) * tile + lanes
    for copy in copies:
        copy.wait()
    summed = lead_part[0]
    for source in range(1, col_count):
        summed = summed + lead_part[source]
    lead_piece[...] = summed
    copies = row_copies(lead_piece, lead_all.at[row_id])
    for copy in copies:
        copy.start()
    lead_all[pl.ds(row_id, 1)] = summed[None]
    for copy in copies:
        copy.wait()
    for owner in range(row_count):
        panel[:, owner * row_tiles : (owner + 1) * row_tiles, :] = lead_all[owner]

    pos = places[...]
    lane = lax.broadcasted_iota(jnp.int32, (1, tile), 1)
    lane3 = lax.broadcasted_iota(jnp.int32, (PB, 1, tile), 2)
    chunk = 64
    rows = row_tiles * tile

    @pl.loop(0, PB)
    def _(step):
        slot = lax.rem(step, 2)
        head_v = jnp.sum(jnp.where(lane3 == step, vecs[:, 0:1, :], 0.0), axis=2, keepdims=True)
        head_w = jnp.sum(jnp.where(lane3 == step, images[:, 0:1, :], 0.0), axis=2, keepdims=True)
        column = panel[step]
        for k in range(PB - 1):
            column = column - vecs[k] * head_w[k] - images[k] * head_v[k]
        below = pos > step + 1
        pivot = total(jnp.where(pos == step + 1, column, 0.0))
        here = total(jnp.where(pos == step, column, 0.0))
        tail = total(jnp.where(below, column * column, 0.0))
        length = jnp.sqrt(pivot * pivot + tail)
        beta = jnp.where(pivot >= 0.0, -length, length)
        tau = (beta - pivot) / beta
        vector = jnp.where(
            pos == step + 1, 1.0, jnp.where(below, column / (pivot - beta), 0.0)
        )
        vector_now[...] = vector
        local = []
        for g in range(col_tiles):
            b = col_id + col_count * g
            local.append(
                vector_now[pl.ds(lax.rem(b, row_count) * row_tiles + lax.div(b, row_count), 1), :]
            )
        for start in range(0, rows, chunk):
            acc = block[start : start + chunk, 0:tile] * local[0]
            for g in range(1, col_tiles):
                acc = acc + block[start : start + chunk, g * tile : (g + 1) * tile] * local[g]
            folded[start : start + chunk, :] = acc
        sums = lax.dot_general(
            jnp.ones((8, tile), jnp.float32),
            folded[...],
            (((1,), (1,)), ((), ())),
            precision=lax.Precision.HIGHEST,
            preferred_element_type=jnp.float32,
        )
        for t in range(row_tiles):
            part[step, row_id, col_id, t : t + 1, :] = sums[0:1, t * tile : (t + 1) * tile]
        sent = all_copies(part.at[step, row_id, col_id], slot)
        for copy in sent:
            copy.start()
        onto_w = [total(images[k] * vector) for k in range(PB - 1)]
        onto_v = [total(vecs[k] * vector) for k in range(PB - 1)]
        fix = vecs[0] * onto_w[0] + images[0] * onto_v[0]
        for k in range(1, PB - 1):
            fix = fix + vecs[k] * onto_w[k] + images[k] * onto_v[k]
        vecs[pl.ds(step, 1)] = vector[None]
        diagonal[...] = jnp.where(lane == step, here, diagonal[...])
        offdiag[...] = jnp.where(lane == step, beta, offdiag[...])
        for copy in sent:
            copy.wait()
        for owner in range(row_count):
            piece = part[step, owner, 0]
            for source in range(1, col_count):
                piece = piece + part[step, owner, source]
            full[owner * row_tiles : (owner + 1) * row_tiles, :] = piece
        image = tau * (full[...] - fix)
        image = image - 0.5 * tau * total(image * vector) * vector
        images[pl.ds(step, 1)] = image[None]


def reduce_panel(block, lead, sizes):
    row_count, col_count, row_tiles, col_tiles, tile = sizes
    all_tiles = row_count * row_tiles
    f32 = jnp.float32
    whole = pl.BlockSpec(memory_space=pltpu.VMEM)
    return pl.pallas_call(
        functools.partial(panel_kernel, sizes),
        out_shape=(
            jax.ShapeDtypeStruct((PB, all_tiles, tile), f32),
            jax.ShapeDtypeStruct((PB, all_tiles, tile), f32),
            jax.ShapeDtypeStruct((1, tile), f32),
            jax.ShapeDtypeStruct((1, tile), f32),
        ),
        in_specs=[whole, whole],
        out_specs=(whole, whole, whole, whole),
        scratch_shapes=[
            pltpu.VMEM((PB, all_tiles, tile), f32),
            pltpu.VMEM((all_tiles, tile), jnp.int32),
            pltpu.VMEM((all_tiles, tile), f32),
            pltpu.VMEM((row_tiles * tile, tile), f32),
            pltpu.VMEM((PB, row_count, col_count, row_tiles, tile), f32),
            pltpu.VMEM((all_tiles, tile), f32),
            pltpu.VMEM((col_count, PB, row_tiles, tile), f32),
            pltpu.VMEM((PB, row_tiles, tile), f32),
            pltpu.VMEM((row_count, PB, row_tiles, tile), f32),
            pltpu.SemaphoreType.DMA((col_count,)),
            pltpu.SemaphoreType.DMA((col_count,)),
            pltpu.SemaphoreType.DMA((row_count,)),
            pltpu.SemaphoreType.DMA((row_count,)),
            pltpu.SemaphoreType.DMA((2, row_count * col_count)),
            pltpu.SemaphoreType.DMA((2, row_count * col_count)),
        ],
        compiler_params=pltpu.CompilerParams(
            collective_id=0, has_side_effects=True, vmem_limit_bytes=24 * 1024 * 1024
        ),
        cost_estimate=pl.CostEstimate(
            flops=400_000_000, bytes_accessed=4_000_000, transcendentals=0
        ),
        name="panel",
    )(block, lead)


def spread_kernel(
    row_count, col_count, rows_in, cols_in, row_all, col_all,
    own_sem, a1_send, a1_recv, a2_send, a2_recv, b1_send, b1_recv,
    right_send, right_recv, left_send, left_recv, pair_send, pair_recv,
):
    row_id = lax.axis_index("row")
    col_id = lax.axis_index("col")
    ring = row_count // 2
    half = ring // 2

    def row_at(shift):
        return lax.rem(row_id + shift + row_count, row_count)

    def col_peer(distance):
        return (row_id, lax.rem(col_id + distance, col_count))

    barrier = pltpu.get_barrier_semaphore()
    for distance in range(1, col_count):
        pl.semaphore_signal(
            barrier, inc=1, device_id=col_peer(distance), device_id_type=pl.DeviceIdType.MESH
        )
    for distance in range(1, row_count):
        pl.semaphore_signal(
            barrier, inc=1, device_id=(row_at(distance), col_id),
            device_id_type=pl.DeviceIdType.MESH,
        )
    pl.semaphore_wait(barrier, row_count + col_count - 2)

    def remote(source, target, send, recv, device):
        return pltpu.make_async_remote_copy(
            src_ref=source, dst_ref=target, send_sem=send, recv_sem=recv,
            device_id=device, device_id_type=pl.DeviceIdType.MESH,
        )

    own = [
        pltpu.make_async_copy(cols_in.at[col_id], col_all.at[:, row_id, col_id], own_sem.at[0]),
        pltpu.make_async_copy(rows_in.at[row_id], row_all.at[:, row_id, col_id], own_sem.at[1]),
    ]
    b1 = []
    for d in range(1, col_count):
        peer = col_peer(d)
        b1.append(remote(
            cols_in.at[peer[1]], col_all.at[:, row_id, col_id], b1_send.at[d], b1_recv.at[d], peer
        ))
    a1 = []
    for d in range(1, row_count):
        peer = row_at(d)
        a1.append(remote(
            rows_in.at[peer], row_all.at[:, row_id, col_id], a1_send.at[d], a1_recv.at[d],
            (peer, col_id),
        ))
    for copy in b1 + own + a1:
        copy.start()
    own[0].wait()
    for copy in b1:
        copy.wait()

    def forward(step, origin, shift, final_part, send, recv):
        place = col_all.at[:, origin] if step < half else col_all.at[final_part, origin]
        return remote(place, place, send.at[step], recv.at[step], (row_at(shift), col_id))

    partner = row_id + 1 - 2 * lax.rem(row_id, 2)

    def to_partner(index, origin):
        place = col_all.at[:, origin]
        return remote(place, place, pair_send.at[index], pair_recv.at[index], (partner, col_id))

    right = [forward(1, row_id, 2, 0, right_send, right_recv)]
    left = [forward(1, row_id, -2, 1, left_send, left_recv)]
    pairs = [to_partner(0, row_id)]
    right[0].start()
    left[0].start()
    pairs[0].start()
    own[1].wait()
    for copy in a1:
        copy.wait()
    a2 = []
    for d in range(1, col_count):
        place = row_all.at[:, :, col_id]
        a2.append(remote(place, place, a2_send.at[d], a2_recv.at[d], col_peer(d)))
        a2[-1].start()
    for step in range(1, half):
        from_left = row_at(-2 * step)
        from_right = row_at(2 * step)
        right[-1].wait_recv()
        right.append(forward(step + 1, from_left, 2, 0, right_send, right_recv))
        right[-1].start()
        left[-1].wait_recv()
        left.append(forward(step + 1, from_right, -2, 1, left_send, left_recv))
        left[-1].start()
        for index, origin in ((2 * step - 1, from_left), (2 * step, from_right)):
            pairs.append(to_partner(index, origin))
            pairs[-1].start()
    right[-1].wait_recv()
    left[-1].wait_recv()
    pairs.append(to_partner(ring - 1, row_at(2 * half)))
    pairs[-1].start()
    for copy in a2:
        copy.wait()
    for copy in pairs:
        copy.wait()
    for copy in right + left:
        copy.wait_send()


def spread(psi, hpsi, row_count, col_count, row_tiles, col_tiles, tile):
    g_rows = psi.shape[0]
    both = jnp.stack([psi, hpsi])
    rows_in = jnp.transpose(
        both.reshape(2, g_rows, row_tiles, row_count, tile), (3, 0, 1, 2, 4)
    ).reshape(row_count, 2, g_rows, row_tiles * tile)
    cols_in = jnp.transpose(
        both.reshape(2, g_rows, col_tiles, col_count, tile), (3, 0, 1, 2, 4)
    ).reshape(col_count, 2, g_rows, col_tiles * tile)
    whole = pl.BlockSpec(memory_space=pltpu.VMEM)
    hbm = pl.BlockSpec(memory_space=pltpu.VMEM)
    ring = row_count // 2
    dma = pltpu.SemaphoreType.DMA
    return pl.pallas_call(
        functools.partial(spread_kernel, row_count, col_count),
        out_shape=(
            jax.ShapeDtypeStruct(
                (2, row_count, col_count, g_rows, row_tiles * tile), psi.dtype
            ),
            jax.ShapeDtypeStruct(
                (2, row_count, col_count, g_rows, col_tiles * tile), psi.dtype
            ),
        ),
        in_specs=[whole, whole],
        out_specs=(hbm, hbm),
        scratch_shapes=[
            dma((2,)),
            dma((row_count,)), dma((row_count,)),
            dma((col_count,)), dma((col_count,)),
            dma((col_count,)), dma((col_count,)),
            dma((ring,)), dma((ring,)), dma((ring,)), dma((ring,)),
            dma((ring,)), dma((ring,)),
        ],
        compiler_params=pltpu.CompilerParams(
            collective_id=1, has_side_effects=True, vmem_limit_bytes=40 * 1024 * 1024
        ),
        cost_estimate=pl.CostEstimate(
            flops=100_000_000, bytes_accessed=8_000_000, transcendentals=0
        ),
        name="spread",
    )(rows_in, cols_in)


def on_device(psi, hpsi, eigvec):
    highest = lax.Precision.HIGHEST
    g_rows = psi.shape[0]
    bands = psi.shape[1]
    row_tiles = eigvec.shape[0]
    tile_size = eigvec.shape[2]
    col_tiles = eigvec.shape[3]
    row_count = lax.axis_size("row")
    col_count = lax.axis_size("col")
    row_id = lax.axis_index("row")
    col_id = lax.axis_index("col")
    gvecs = g_rows * row_count * col_count
    row_width = row_tiles * tile_size
    col_width = col_tiles * tile_size
    row_all, col_all = spread(
        psi, hpsi, row_count, col_count, row_tiles, col_tiles, tile_size
    )
    psi_rows = row_all[0].reshape(gvecs, row_width)
    hpsi_rows = row_all[1].reshape(gvecs, row_width)
    psi_cols = col_all[0].reshape(gvecs, col_width)
    hpsi_cols = col_all[1].reshape(gvecs, col_width)
    reduced = 0.5 * (inner(psi_rows, hpsi_cols) + inner(hpsi_rows, psi_cols))
    correlation = inner(psi_rows, psi_cols) / float(gvecs)
    blocks = reduced.reshape(row_tiles, tile_size, col_tiles, tile_size)
    leading = blocks[:, :, 0, :PB]
    lead = jnp.where(col_id == 0, jnp.transpose(leading, (2, 0, 1)), 0.0)
    sizes = (row_count, col_count, row_tiles, col_tiles, tile_size)
    vecs, images, diagonal, offdiag = reduce_panel(reduced, lead, sizes)
    diagonal = diagonal[0, :PB]
    offdiag = offdiag[0, :PB]

    def rows_of(matrix):
        return lax.dynamic_index_in_dim(
            matrix.reshape(PB, row_count, row_tiles, tile_size), row_id, 1, keepdims=False
        ).reshape(PB, row_width)

    def cols_of(matrix):
        ordered = jnp.transpose(
            matrix.reshape(PB, row_count, row_tiles, tile_size), (0, 2, 1, 3)
        )
        return lax.dynamic_index_in_dim(
            ordered.reshape(PB, col_tiles, col_count, tile_size), col_id, 2, keepdims=False
        ).reshape(PB, col_width)

    left = jnp.concatenate([rows_of(vecs), rows_of(images)], axis=0)
    right = jnp.concatenate([cols_of(images), cols_of(vecs)], axis=0)
    updated = reduced - lax.dot_general(
        left, right, (((0,), (0,)), ((), ())), precision=highest,
        preferred_element_type=jnp.float32,
    )
    flat = eigvec.reshape(row_width, col_width)
    rotated = lax.psum_scatter(
        jnp.dot(psi_rows, flat, preferred_element_type=jnp.float32),
        "row",
        scatter_dimension=0,
        tiled=True,
    )
    tile_shape = (row_tiles, 1, tile_size, col_tiles, 1, tile_size)
    return (
        correlation.reshape(tile_shape),
        updated.reshape(tile_shape),
        diagonal,
        offdiag,
        rotated.astype(jnp.bfloat16).reshape(rotated.shape[0], col_tiles, 1, tile_size),
    )


def solution(mesh):
    return jax.shard_map(
        on_device,
        mesh=mesh,
        in_specs=(
            P(("row", "col"), None),
            P(("row", "col"), None),
            P(None, "row", None, None, "col", None),
        ),
        out_specs=(
            P(None, "row", None, None, "col", None),
            P(None, "row", None, None, "col", None),
            P(),
            P(),
            P("row", None, "col", None),
        ),
        check_vma=False,
    )
```
